32 devices in a mesh: part: 1 (over z), dp: 32 (over y, x, core).
Axes of the slice: x: 4, y: 4, z: 1, core: 2. Of those that a mesh axis runs over, the one named last changes fastest.
The devices are a block of a 4x4x8 slice.
Arguments:
- tokens: bfloat16 [96, 384, 2048], P(('part', 'dp'))
- lengths: int32 [96], P(('part', 'dp'))
- ln1_gain: bfloat16 [2, 2048], P(None, 'dp')
- ln1_bias: bfloat16 [2, 2048], P(None, 'dp')
- w_attn: bfloat16 [2, 2048, 2304], P(None, 'dp')
- b_attn: bfloat16 [2, 2304], P(None, 'dp')
- w_out: bfloat16 [2, 2048, 2048], P(None, 'dp')
- b_out: bfloat16 [2, 2048], P(None, 'dp')
- ln2_gain: bfloat16 [2, 2048], P(None, 'dp')
- ln2_bias: bfloat16 [2, 2048], P(None, 'dp')
- w_fc: bfloat16 [2, 2048, 8192], P(None, 'dp')
- b_fc: bfloat16 [2, 8192], P(None, 'dp')
- w_proj: bfloat16 [2, 8192, 2048], P(None, 'dp')
- b_proj: bfloat16 [2, 2048], P(None, 'dp')
Outputs:
- output 1: bfloat16 [96, 384, 2048], P(('part', 'dp'))
- output 2: bfloat16 [96, 2, 384, 128], P(('part', 'dp'))
- output 3: bfloat16 [96, 2, 384, 128], P(('part', 'dp'))
All inputs are finite; a program needn't handle non-finite values.
Results may differ from the reference program's by a relative error of at most 0.0192267.
Values are sent between devices in bfloat16 or wider.
A program may use at most 768 MiB of HBM per device.

```python
import jax
import jax.numpy as jnp
from jax import lax

D = 2048
HEADS = 16
HEAD = 128
FF = 8192
SEQ = 384
PROMPTS = 96
LAYERS = 2
EPS = 1e-5
QKV = D + 2 * HEAD


def draw(key, shape, scale, offset):
    return (offset + scale * jax.random.normal(key, shape, jnp.float32)).astype(jnp.bfloat16)


def setup_inputs(seed: int = 0, part: int = 0) -> dict:
    shared = jax.random.split(jax.random.key(seed), 12)
    own = jax.random.split(jax.random.fold_in(jax.random.key(seed), part), 2)
    lengths = jax.random.randint(own[1], (PROMPTS,), SEQ // 4, SEQ + 1, dtype=jnp.int32)
    lengths = lengths.at[0].set(SEQ).at[1].set(SEQ // 4)
    qkv_scale = jnp.concatenate([jnp.full((D + HEAD,), 2.0, jnp.float32), jnp.ones((HEAD,), jnp.float32)]) * D ** -0.5
    return dict(
        tokens=draw(own[0], (PROMPTS, SEQ, D), 1.0, 0.0),
        lengths=lengths,
        ln1_gain=draw(shared[0], (LAYERS, D), 0.3, 1.0),
        ln1_bias=draw(shared[1], (LAYERS, D), 0.3, 0.0),
        w_attn=draw(shared[2], (LAYERS, D, QKV), qkv_scale, 0.0),
        b_attn=draw(shared[3], (LAYERS, QKV), 0.3, 0.0),
        w_out=draw(shared[4], (LAYERS, D, D), D ** -0.5, 0.0),
        b_out=draw(shared[5], (LAYERS, D), 0.3, 0.0),
        ln2_gain=draw(shared[6], (LAYERS, D), 0.3, 1.0),
        ln2_bias=draw(shared[7], (LAYERS, D), 0.3, 0.0),
        w_fc=draw(shared[8], (LAYERS, D, FF), D ** -0.5, 0.0),
        b_fc=draw(shared[9], (LAYERS, FF), 0.3, 0.0),
        w_proj=draw(shared[10], (LAYERS, FF, D), FF ** -0.5, 0.0),
        b_proj=draw(shared[11], (LAYERS, D), 0.3, 0.0),
    )


def layer_norm(values, gain, shift):
    wide = values.astype(jnp.float32)
    mean = jnp.mean(wide, axis=-1, keepdims=True)
    centred = wide - mean
    variance = jnp.mean(centred * centred, axis=-1, keepdims=True)
    normed = centred * lax.rsqrt(variance + EPS)
    return (normed * gain.astype(jnp.float32) + shift.astype(jnp.float32)).astype(jnp.bfloat16)


def attend(query, keys, values, length):
    q_heads = query.reshape(SEQ, HEADS, HEAD).astype(jnp.float32)
    scores = jnp.einsum('shd,td->sht', q_heads, keys.astype(jnp.float32)) * HEAD ** -0.5
    position = jnp.arange(SEQ)
    allowed = (position[None, :] <= position[:, None]) & (position[None, :] < length)
    scores = jnp.where(allowed[:, None, :], scores, -1e30)
    attn_prob = jax.nn.softmax(scores, axis=-1).astype(jnp.bfloat16).astype(jnp.float32)
    mixed = jnp.einsum('sht,td->shd', attn_prob, values.astype(jnp.float32))
    return mixed.astype(jnp.bfloat16).reshape(SEQ, D)


def block(state, length, params):
    ln1_gain, ln1_bias, w_attn, b_attn, w_out, b_out, ln2_gain, ln2_bias, w_fc, b_fc, w_proj, b_proj = params
    hidden = layer_norm(state, ln1_gain, ln1_bias)
    qkv_all = (jnp.dot(hidden, w_attn, preferred_element_type=jnp.float32) + b_attn.astype(jnp.float32)).astype(jnp.bfloat16)
    keys = qkv_all[:, D:D + HEAD]
    values = qkv_all[:, D + HEAD:]
    attended = attend(qkv_all[:, :D], keys, values, length)
    residual = (state.astype(jnp.float32) + jnp.dot(attended, w_out, preferred_element_type=jnp.float32) + b_out.astype(jnp.float32)).astype(jnp.bfloat16)
    hidden2 = layer_norm(residual, ln2_gain, ln2_bias)
    inner = jax.nn.gelu(jnp.dot(hidden2, w_fc, preferred_element_type=jnp.float32) + b_fc.astype(jnp.float32), approximate=True).astype(jnp.bfloat16)
    updated = (residual.astype(jnp.float32) + jnp.dot(inner, w_proj, preferred_element_type=jnp.float32) + b_proj.astype(jnp.float32)).astype(jnp.bfloat16)
    return updated, keys, values


def reference(tokens, lengths, ln1_gain, ln1_bias, w_attn, b_attn, w_out, b_out, ln2_gain, ln2_bias, w_fc, b_fc, w_proj, b_proj):
    params = (ln1_gain, ln1_bias, w_attn, b_attn, w_out, b_out, ln2_gain, ln2_bias, w_fc, b_fc, w_proj, b_proj)

    def one_prompt(item):
        prompt, length = item

        def step(state, layer_params):
            updated, keys, values = block(state, length, layer_params)
            return updated, (keys, values)

        final, caches = lax.scan(step, prompt, params)
        return final, caches[0], caches[1]

    out_tokens, k_cache, v_cache = lax.map(one_prompt, (tokens, lengths))
    return out_tokens, k_cache, v_cache
```

```python
import functools
import math

import jax
import jax.numpy as jnp
from jax import lax
from jax.experimental import pallas as pl
from jax.experimental.pallas import tpu as pltpu
from jax.sharding import PartitionSpec as P

EPS = 1e-5
F32 = jnp.float32
BF16 = jnp.bfloat16
FC_PARTS = 4
PROJ_PARTS = 4
VROWS = 16
VCOLS = 256
RUN_COMM = True
RUN_COMPUTE = True

LN1G, LN1B, LN2G, LN2B, BOUT, BPROJ, BATTN, BFC = range(8)


def fori(lower, upper, body):
    lax.fori_loop(lower, upper, lambda i, c: (body(i), c)[1], 0)


def kernel(n, tok, lens, ln1g, ln1b, b_attn, b_out, ln2g, ln2b, b_fc, b_proj, w_attn, w_out, w_fc, w_proj,
           out, kc, vc, g_vec, g_attn, g_main, g_proj,
           x, h, inner, wa, wm, wp, vecs, vp, vp16, gv,
           recv, d2d, sent, load_sem, io_sem, cache_sem):
    layers = w_attn.shape[0]
    prompts, seq, width = tok.shape
    head = kc.shape[-1]
    heads = width // head
    ff = b_fc.shape[1] * n
    tokens = prompts * seq
    qkv = width + 2 * head
    per_layer = 2 + FC_PARTS + PROJ_PARTS
    chunks = 1 + layers * per_layer
    fc_cols = ff // FC_PARTS
    pr_cols = width // PROJ_PARTS

    side = math.isqrt(n // 2)
    me = lax.axis_index("dp")
    core = me % 2
    px = (me // 2) % side
    py = me // (2 * side)

    def dev(dx, dy):
        return (((py + dy + side) % side) * side + (px + dx + side) % side) * 2 + core

    sibling = me + 1 - 2 * core
    xp, xm, yp, ym = dev(1, 0), dev(-1, 0), dev(0, 1), dev(0, -1)

    def owner(dx, dy):
        return dev(-dx, -dy)

    vp[...] = jnp.zeros_like(vp)
    for k, ref in ((LN1G, ln1g), (LN1B, ln1b), (LN2G, ln2g), (LN2B, ln2b), (BOUT, b_out), (BPROJ, b_proj), (BATTN, b_attn), (BFC, b_fc)):
        wide = ref[...].astype(F32)
        for layer in range(layers):
            vp[layer * VROWS + k:layer * VROWS + k + 1, 0:ref.shape[1]] = wide[layer:layer + 1, :]
    vp16[...] = vp[...].astype(BF16)

    for p in range(prompts):
        pltpu.make_async_copy(tok.at[p], x.at[pl.ds(p * seq, seq), :], io_sem.at[p]).start()

    barrier = pltpu.get_barrier_semaphore()
    for other in (xp, xm, yp, ym, sibling):
        pl.semaphore_signal(barrier, inc=1, device_id={"dp": other})
    pl.semaphore_wait(barrier, 5)

    def layer_of(j):
        return (j - 1) // per_layer, (j - 1) % per_layer

    def by_kind(j, fn):
        layer, r = layer_of(j)

        @pl.when(j == 0)
        def _():
            fn(g_vec)

        @pl.when((j > 0) & (r == 0))
        def _():
            fn(g_attn.at[layer])

        @pl.when((j > 0) & (r >= 1) & (r < 2 + FC_PARTS))
        def _():
            fn(g_main.at[layer, r - 1])

        @pl.when((j > 0) & (r >= 2 + FC_PARTS))
        def _():
            fn(g_proj.at[layer, r - 2 - FC_PARTS])

    def own_by_kind(j, fn):
        layer, r = layer_of(j)

        @pl.when(j == 0)
        def _():
            fn(vp16, g_vec)

        @pl.when((j > 0) & (r == 0))
        def _():
            fn(w_attn.at[layer], g_attn.at[layer])

        @pl.when((j > 0) & (r == 1))
        def _():
            fn(w_out.at[layer], g_main.at[layer, 0])

        @pl.when((j > 0) & (r >= 2) & (r < 2 + FC_PARTS))
        def _():
            c = r - 2
            fn(w_fc.at[layer, :, pl.ds(pl.multiple_of(c * fc_cols, fc_cols), fc_cols)], g_main.at[layer, r - 1])

        @pl.when((j > 0) & (r >= 2 + FC_PARTS))
        def _():
            c = r - 2 - FC_PARTS
            fn(w_proj.at[layer, :, pl.ds(pl.multiple_of(c * pr_cols, pr_cols), pr_cols)], g_proj.at[layer, c])

    def wait_shards(view, count, sem):
        part = view.at[pl.ds(0, count)]
        pltpu.make_async_copy(part, part, sem).wait()

    def push(src, dst, j, sem, device):
        pltpu.make_async_remote_copy(src_ref=src, dst_ref=dst, send_sem=sent.at[j], recv_sem=sem, device_id={"dp": device}).start()

    def relay(view, j, event, moves):
        rows, cols = view.shape[1], view.shape[2]
        half_r, half_c = rows // 2, cols // 2
        whole_r, whole_c = pl.ds(0, rows), pl.ds(0, cols)
        top, bottom = pl.ds(0, half_r), pl.ds(half_r, half_r)
        left, right = pl.ds(0, half_c), pl.ds(half_c, half_c)
        cut = dict(top=(top, whole_c), bottom=(bottom, whole_c), left=(whole_r, left), right=(whole_r, right),
                   a=(top, left), b=(top, right), c=(bottom, left), d=(bottom, right))
        for (dx, dy), name, target in moves:
            block = view.at[owner(dx, dy)].at[cut[name]]
            push(block, block, j, recv.at[event, j], target)

    def hand_over(view, j, offsets):
        for dx, dy in offsets:
            block = view.at[owner(dx, dy)]
            push(block, block, j, d2d.at[j], sibling)

    def event0(j):
        def go(src, view):
            for target in (xp, xm, yp, ym):
                push(src, view.at[me], j, recv.at[0, j], target)
            push(src, view.at[me], j, d2d.at[j], sibling)
        own_by_kind(j, go)

    def event1(j):
        def go(view):
            wait_shards(view, 4, recv.at[0, j])
            relay(view, j, 1, (
                ((1, 0), "left", xp), ((-1, 0), "right", xm), ((0, 1), "left", yp), ((0, -1), "right", ym),
                ((0, 1), "bottom", xp), ((0, 1), "bottom", xm), ((1, 0), "top", yp), ((1, 0), "top", ym),
                ((0, -1), "bottom", xp), ((0, -1), "bottom", xm), ((-1, 0), "top", yp), ((-1, 0), "top", ym)))
            hand_over(view, j, ((1, 0), (-1, 0), (0, 1), (0, -1)))
        by_kind(j, go)

    def event2(j):
        def go(view):
            wait_shards(view, 6, recv.at[1, j])
            relay(view, j, 2, (
                ((0, 2), "bottom", xp), ((0, 2), "bottom", xm), ((2, 0), "top", yp), ((2, 0), "top", ym),
                ((1, 1), "c", xp), ((-1, 1), "d", xm), ((1, 1), "a", yp), ((1, -1), "b", ym),
                ((1, -1), "c", xp), ((-1, -1), "d", xm), ((-1, 1), "a", yp), ((-1, -1), "b", ym)))
            hand_over(view, j, ((2, 0), (0, 2), (1, 1), (1, -1), (-1, 1), (-1, -1)))
        by_kind(j, go)

    def event3(j):
        def go(view):
            wait_shards(view, 4, recv.at[2, j])
            relay(view, j, 3, (((1, 2), "c", xp), ((-1, 2), "d", xm), ((2, 1), "a", yp), ((2, -1), "b", ym)))
            hand_over(view, j, ((2, 1), (2, -1), (1, 2), (-1, 2)))
        by_kind(j, go)

    def event4(j):
        def go(view):
            wait_shards(view, 1, recv.at[3, j])
            hand_over(view, j, ((2, 2),))
        by_kind(j, go)

    def pump(t):
        for event, shift in ((event4, -1), (event3, 0), (event2, 1), (event1, 2), (event0, 3)):
            j = t + shift
            pl.when((j >= 0) & (j < chunks))(functools.partial(event, j))

    def load(view, own, slot, j):
        rows = view.shape[1]
        if RUN_COMM:
            wait_shards(view, n // 2, d2d.at[j])

        def one(d):
            place = slot.at[pl.ds(pl.multiple_of(d * rows, rows), rows), :]

            @pl.when(d != me)
            def _():
                pltpu.make_async_copy(view.at[d], place, load_sem).start()

            @pl.when(d == me)
            def _():
                pltpu.make_async_copy(own, place, load_sem).start()

        fori(0, n, one)
        pltpu.make_async_copy(slot, slot, load_sem).wait()

    def spread_vectors():
        load(g_vec, vp16, gv, 0)
        rows = gv.shape[0]
        for layer in range(layers):
            for k, part, total in ((LN1G, width // n, width), (LN1B, width // n, width), (LN2G, width // n, width),
                                   (LN2B, width // n, width), (BOUT, width // n, width), (BPROJ, width // n, width),
                                   (BATTN, qkv // n, qkv), (BFC, ff // n, ff)):
                dd = lax.broadcasted_iota(jnp.int32, (n, rows), 0)
                rr = lax.broadcasted_iota(jnp.int32, (n, rows), 1)
                pick = jnp.where(rr == dd * (2 * VROWS) + (layer * VROWS + k), 1.0, 0.0).astype(BF16)
                piece = jnp.dot(pick, gv[...], preferred_element_type=F32).astype(BF16)
                block = total if total <= qkv else width
                for start in range(0, total, block):
                    pos = lax.broadcasted_iota(jnp.int32, (1, block), 1).astype(F32) + float(start)
                    whose = jnp.floor((pos + 0.5) * (1.0 / part))
                    lane = pos - whose * float(part)
                    cc = lax.broadcasted_iota(jnp.int32, (VCOLS, block), 0).astype(F32)
                    place = jnp.where(cc == lane, 1.0, 0.0).astype(BF16)
                    wide = jnp.dot(piece, place, preferred_element_type=F32)
                    di = lax.broadcasted_iota(jnp.int32, (n, block), 0).astype(F32)
                    row = jnp.sum(jnp.where(di == whose, wide, 0.0), axis=0, keepdims=True)
                    vecs[layer, k:k + 1, start:start + block] = row

    def layer_norm(layer, gain_row, shift_row):
        tile = 16

        def one(m):
            rows = pl.ds(pl.multiple_of(m * tile, tile), tile)
            wide = x[rows, :].astype(F32)
            mean = jnp.mean(wide, axis=-1, keepdims=True)
            centred = wide - mean
            variance = jnp.mean(centred * centred, axis=-1, keepdims=True)
            normed = centred * lax.rsqrt(variance + EPS)
            gain = vecs[layer, gain_row:gain_row + 1, 0:width]
            shift = vecs[layer, shift_row:shift_row + 1, 0:width]
            h[rows, :] = (normed * gain + shift).astype(BF16)

        fori(0, tokens // tile, one)

    m_tile = seq

    def stage_qkv(layer):
        load(g_attn.at[layer], w_attn.at[layer], wa, 1 + layer * per_layer)
        layer_norm(layer, LN1G, LN1B)
        n_tile = 2 * head

        def one(i):
            cols = pl.ds(pl.multiple_of(i * n_tile, n_tile), n_tile)
            bias = vecs[layer, BATTN:BATTN + 1, cols]
            for m in range(tokens // m_tile):
                rows = slice(m * m_tile, (m + 1) * m_tile)
                acc = jnp.dot(h[rows, :], wa[:, cols], preferred_element_type=F32)
                inner[rows, cols] = (acc + bias).astype(BF16)

        fori(0, qkv // n_tile, one)
        for p in range(prompts):
            rows = pl.ds(p * seq, seq)
            pltpu.make_async_copy(inner.at[rows, pl.ds(width, head)], kc.at[p, layer], cache_sem.at[2 * p]).start()
            pltpu.make_async_copy(inner.at[rows, pl.ds(width + head, head)], vc.at[p, layer], cache_sem.at[2 * p + 1]).start()

    def wait_caches(layer):
        for p in range(prompts):
            rows = pl.ds(p * seq, seq)
            pltpu.make_async_copy(inner.at[rows, pl.ds(width, head)], kc.at[p, layer], cache_sem.at[2 * p]).wait()
            pltpu.make_async_copy(inner.at[rows, pl.ds(width + head, head)], vc.at[p, layer], cache_sem.at[2 * p + 1]).wait()

    q_tile = 128
    scale = head ** -0.5

    def attention(p):
        length = lens[p]
        unroll = 2

        def one(i):
            for u in range(unroll):
                cols = pl.ds(pl.multiple_of((i * unroll + u) * head, head), head)
                for b in range(seq // q_tile):
                    keys = (b + 1) * q_tile
                    rows = slice(p * seq + b * q_tile, p * seq + (b + 1) * q_tile)
                    query = inner[rows, cols]
                    kk = inner[p * seq:p * seq + keys, width:width + head]
                    vv = inner[p * seq:p * seq + keys, width + head:width + 2 * head]
                    score = lax.dot_general(query, kk, (((1,), (1,)), ((), ())), preferred_element_type=F32) * scale
                    ki = lax.broadcasted_iota(jnp.int32, (q_tile, keys), 1)
                    qi = lax.broadcasted_iota(jnp.int32, (q_tile, keys), 0) + b * q_tile
                    score = jnp.where((ki <= qi) & (ki < length), score, -1e30)
                    peak = jnp.max(score, axis=-1, keepdims=True)
                    e = jnp.exp(score - peak)
                    prob = (e / jnp.sum(e, axis=-1, keepdims=True)).astype(BF16)
                    mixed = jnp.dot(prob, vv, preferred_element_type=F32)
                    h[rows, cols] = mixed.astype(BF16)

        fori(0, heads // unroll, one)

    def stage_out(layer):
        load(g_main.at[layer, 0], w_out.at[layer], wm, 2 + layer * per_layer)
        n_tile = min(512, width)

        def one(i):
            cols = pl.ds(pl.multiple_of(i * n_tile, n_tile), n_tile)
            bias = vecs[layer, BOUT:BOUT + 1, cols]
            for m in range(tokens // m_tile):
                rows = slice(m * m_tile, (m + 1) * m_tile)
                acc = jnp.dot(h[rows, :], wm[:, cols], preferred_element_type=F32)
                x[rows, cols] = (x[rows, cols].astype(F32) + (acc + bias)).astype(BF16)

        fori(0, width // n_tile, one)
        layer_norm(layer, LN2G, LN2B)

    def stage_fc(layer, c):
        base = c * fc_cols
        load(g_main.at[layer, 1 + c], w_fc.at[layer, :, pl.ds(pl.multiple_of(base, fc_cols), fc_cols)], wm,
             3 + c + layer * per_layer)
        n_tile = min(512, fc_cols)

        def one(i):
            cols = pl.ds(pl.multiple_of(i * n_tile, n_tile), n_tile)
            far = pl.ds(pl.multiple_of(base + i * n_tile, n_tile), n_tile)
            bias = vecs[layer, BFC:BFC + 1, far]
            for m in range(tokens // m_tile):
                rows = slice(m * m_tile, (m + 1) * m_tile)
                acc = jnp.dot(h[rows, :], wm[:, cols], preferred_element_type=F32) + bias
                inner[rows, far] = jax.nn.gelu(acc, approximate=True).astype(BF16)

        fori(0, fc_cols // n_tile, one)

    def stage_proj(layer, c):
        base = c * pr_cols
        cols = pl.ds(pl.multiple_of(base, pr_cols), pr_cols)
        load(g_proj.at[layer, c], w_proj.at[layer, :, cols], wp, 3 + FC_PARTS + c + layer * per_layer)
        bias = vecs[layer, BPROJ:BPROJ + 1, cols]

        def one(m):
            rows = pl.ds(pl.multiple_of(m * m_tile, m_tile), m_tile)
            acc = jnp.dot(inner[rows, :], wp[...], preferred_element_type=F32)
            x[rows, cols] = (x[rows, cols].astype(F32) + (acc + bias)).astype(BF16)

        fori(0, tokens // m_tile, one)

    def compute(t):
        layer, r = (t - 2) // per_layer, (t - 2) % per_layer
        live = (t >= 2) & (t < 2 + layers * per_layer)

        @pl.when(t == 1)
        def _():
            spread_vectors()
            for p in range(prompts):
                pltpu.make_async_copy(tok.at[p], x.at[pl.ds(p * seq, seq), :], io_sem.at[p]).wait()

        @pl.when(live & (r == 0))
        def _():
            stage_qkv(layer)

        @pl.when(live & (r == 1))
        def _():
            for p in range(prompts - 1):
                attention(p)

        @pl.when(live & (r == 2))
        def _():
            attention(prompts - 1)
            wait_caches(layer)
            stage_out(layer)

        first_fc = 3

        @pl.when(live & (r >= first_fc) & (r < first_fc + FC_PARTS))
        def _():
            stage_fc(layer, r - first_fc)

        first_proj = first_fc + FC_PARTS
        for_proj = r - first_proj

        @pl.when(live & (r >= first_proj))
        def _():
            lo = jnp.where(for_proj == 2, PROJ_PARTS - 1, for_proj)
            hi = jnp.where(for_proj == 0, 1, jnp.where(for_proj == 1, PROJ_PARTS - 1, PROJ_PARTS))
            fori(lo, hi, lambda c: stage_proj(layer, c))

    def slot_step(i):
        t = i - 3
        if RUN_COMM:
            pump(t)
        if RUN_COMPUTE:
            compute(t)

    fori(0, chunks + 4, slot_step)

    for p in range(prompts):
        pltpu.make_async_copy(x.at[pl.ds(p * seq, seq), :], out.at[p], io_sem.at[p]).start()
    if not RUN_COMPUTE and RUN_COMM:
        fori(0, chunks, lambda j: by_kind(j, lambda view: wait_shards(view, n // 2, d2d.at[j])))
    if RUN_COMM:
        fori(0, chunks, lambda j: by_kind(j, lambda view: wait_shards(view, n - 1, sent.at[j])))
    for p in range(prompts):
        pltpu.make_async_copy(x.at[pl.ds(p * seq, seq), :], out.at[p], io_sem.at[p]).wait()


def solution(mesh):
    n = mesh.shape["dp"]
    tok_spec = P(('part', 'dp'), None, None)
    len_spec = P(('part', 'dp'))
    cache_spec = P(('part', 'dp'), None, None, None)
    vec_spec = P(None, 'dp')
    mat_spec = P(None, 'dp', None)

    def local(tokens, lengths, ln1_gain, ln1_bias, w_attn, b_attn, w_out, b_out, ln2_gain, ln2_bias, w_fc, b_fc, w_proj, b_proj):
        layers = w_attn.shape[0]
        prompts, seq, width = tokens.shape
        qkv = w_attn.shape[2]
        head = (qkv - width) // 2
        ff = w_fc.shape[2]
        rows = prompts * seq
        per_layer = 2 + FC_PARTS + PROJ_PARTS
        chunks = 1 + layers * per_layer
        r_in, r_ff = width // n, ff // n
        assert ff // FC_PARTS == width and layers * VROWS <= 2 * VROWS
        anywhere = pl.BlockSpec(memory_space=pl.ANY)
        vmem = pl.BlockSpec(memory_space=pltpu.VMEM)
        smem = pl.BlockSpec(memory_space=pltpu.SMEM)
        sds = jax.ShapeDtypeStruct
        cache = sds((prompts, layers, seq, head), BF16)
        results = pl.pallas_call(
            functools.partial(kernel, n),
            out_shape=(sds(tokens.shape, BF16), cache, cache,
                       sds((n, 2 * VROWS, VCOLS), BF16),
                       sds((layers, n, r_in, qkv), BF16),
                       sds((layers, 1 + FC_PARTS, n, r_in, width), BF16),
                       sds((layers, PROJ_PARTS, n, r_ff, width // PROJ_PARTS), BF16)),
            in_specs=[anywhere, smem] + [vmem] * 8 + [anywhere] * 4,
            out_specs=(anywhere,) * 7,
            scratch_shapes=[
                pltpu.VMEM((rows, width), BF16),
                pltpu.VMEM((rows, width), BF16),
                pltpu.VMEM((rows, ff), BF16),
                pltpu.VMEM((width, qkv), BF16),
                pltpu.VMEM((width, width), BF16),
                pltpu.VMEM((ff, width // PROJ_PARTS), BF16),
                pltpu.VMEM((layers, 8, ff), F32),
                pltpu.VMEM((2 * VROWS, VCOLS), F32),
                pltpu.VMEM((2 * VROWS, VCOLS), BF16),
                pltpu.VMEM((n * 2 * VROWS, VCOLS), BF16),
                pltpu.SemaphoreType.DMA((4, chunks)),
                pltpu.SemaphoreType.DMA((chunks,)),
                pltpu.SemaphoreType.DMA((chunks,)),
                pltpu.SemaphoreType.DMA,
                pltpu.SemaphoreType.DMA((prompts,)),
                pltpu.SemaphoreType.DMA((2 * prompts,)),
            ],
            compiler_params=pltpu.CompilerParams(collective_id=0, has_side_effects=True, vmem_limit_bytes=67043328),
            name="gather_layers",
        )(tokens, lengths, ln1_gain, ln1_bias, b_attn, b_out, ln2_gain, ln2_bias, b_fc, b_proj, w_attn, w_out, w_fc, w_proj)
        return results[0], results[1], results[2]

    return jax.shard_map(local, mesh=mesh,
                         in_specs=(tok_spec, len_spec, vec_spec, vec_spec, mat_spec, vec_spec, mat_spec, vec_spec, vec_spec, vec_spec, mat_spec, vec_spec, mat_spec, vec_spec),
                         out_specs=(tok_spec, cache_spec, cache_spec), check_vma=False)
```

```python
import functools
import math

import jax
import jax.numpy as jnp
from jax import lax
from jax.experimental import pallas as pl
from jax.experimental.pallas import tpu as pltpu
from jax.sharding import PartitionSpec as P

EPS = 1e-5
F32 = jnp.float32
BF16 = jnp.bfloat16
FC_PARTS = 4
PROJ_PARTS = 4
VROWS = 16
VCOLS = 256
SLOTS = 3
LATE = 3
RUN_COMM = True
RUN_COMPUTE = True

LN1G, LN1B, LN2G, LN2B, BOUT, BPROJ, BATTN, BFC = range(8)


def fori(lower, upper, body):
    lax.fori_loop(lower, upper, lambda i, c: (body(i), c)[1], 0)


def kernel(n, tok, lens, ln1g, ln1b, b_attn, b_out, ln2g, ln2b, b_fc, b_proj, w_attn, w_out, w_fc, w_proj,
           out, kc, vc, g_vec, g_attn, g_main, g_proj,
           x, h, inner, ws, vecs, vp, vp16, gv,
           recv, d2d, sent, load_sem, vec_sem, io_sem, cache_sem):
    layers = w_attn.shape[0]
    prompts, seq, width = tok.shape
    head = kc.shape[-1]
    heads = width // head
    ff = b_fc.shape[1] * n
    tokens = prompts * seq
    qkv = width + 2 * head
    per_layer = 2 + FC_PARTS + PROJ_PARTS
    chunks = 1 + layers * per_layer
    fc_cols = ff // FC_PARTS
    pr_cols = width // PROJ_PARTS

    side = math.isqrt(n // 2)
    me = lax.axis_index("dp")
    core = me % 2
    px = (me // 2) % side
    py = me // (2 * side)

    def dev(dx, dy):
        return (((py + dy + side) % side) * side + (px + dx + side) % side) * 2 + core

    sibling = me + 1 - 2 * core
    xp, xm, yp, ym = dev(1, 0), dev(-1, 0), dev(0, 1), dev(0, -1)

    def owner(dx, dy):
        return dev(-dx, -dy)

    vp[...] = jnp.zeros_like(vp)
    for k, ref in ((LN1G, ln1g), (LN1B, ln1b), (LN2G, ln2g), (LN2B, ln2b), (BOUT, b_out), (BPROJ, b_proj), (BATTN, b_attn), (BFC, b_fc)):
        wide = ref[...].astype(F32)
        for layer in range(layers):
            vp[layer * VROWS + k:layer * VROWS + k + 1, 0:ref.shape[1]] = wide[layer:layer + 1, :]
    vp16[...] = vp[...].astype(BF16)

    for p in range(prompts):
        pltpu.make_async_copy(tok.at[p], x.at[pl.ds(p * seq, seq), :], io_sem.at[p]).start()

    barrier = pltpu.get_barrier_semaphore()
    for other in (xp, xm, yp, ym, sibling):
        pl.semaphore_signal(barrier, inc=1, device_id={"dp": other})
    pl.semaphore_wait(barrier, 5)

    def layer_of(j):
        return (j - 1) // per_layer, (j - 1) % per_layer

    def by_kind(j, fn):
        layer, r = layer_of(j)

        @pl.when(j == 0)
        def _():
            fn(g_vec)

        @pl.when((j > 0) & (r == 0))
        def _():
            fn(g_attn.at[layer])

        @pl.when((j > 0) & (r >= 1) & (r < 2 + FC_PARTS))
        def _():
            fn(g_main.at[layer, r - 1])

        @pl.when((j > 0) & (r >= 2 + FC_PARTS))
        def _():
            fn(g_proj.at[layer, r - 2 - FC_PARTS])

    def own_by_kind(j, fn, vectors=True):
        layer, r = layer_of(j)

        if vectors:
            @pl.when(j == 0)
            def _():
                fn(vp16, g_vec)

        @pl.when((j > 0) & (r == 0))
        def _():
            fn(w_attn.at[layer], g_attn.at[layer])

        @pl.when((j > 0) & (r == 1))
        def _():
            fn(w_out.at[layer], g_main.at[layer, 0])

        @pl.when((j > 0) & (r >= 2) & (r < 2 + FC_PARTS))
        def _():
            c = r - 2
            fn(w_fc.at[layer, :, pl.ds(pl.multiple_of(c * fc_cols, fc_cols), fc_cols)], g_main.at[layer, r - 1])

        @pl.when((j > 0) & (r >= 2 + FC_PARTS))
        def _():
            c = r - 2 - FC_PARTS
            fn(w_proj.at[layer, :, pl.ds(pl.multiple_of(c * pr_cols, pr_cols), pr_cols)], g_proj.at[layer, c])

    def wait_shards(view, count, sem):
        part = view.at[pl.ds(0, count)]
        pltpu.make_async_copy(part, part, sem).wait()

    def push(src, dst, j, sem, device):
        pltpu.make_async_remote_copy(src_ref=src, dst_ref=dst, send_sem=sent.at[j], recv_sem=sem, device_id={"dp": device}).start()

    def relay(view, j, event, moves):
        rows, cols = view.shape[1], view.shape[2]
        half_r, half_c = rows // 2, cols // 2
        whole_r, whole_c = pl.ds(0, rows), pl.ds(0, cols)
        top, bottom = pl.ds(0, half_r), pl.ds(half_r, half_r)
        left, right = pl.ds(0, half_c), pl.ds(half_c, half_c)
        cut = dict(top=(top, whole_c), bottom=(bottom, whole_c), left=(whole_r, left), right=(whole_r, right),
                   a=(top, left), b=(top, right), c=(bottom, left), d=(bottom, right))
        for (dx, dy), name, target in moves:
            block = view.at[owner(dx, dy)].at[cut[name]]
            push(block, block, j, recv.at[event, j], target)

    def hand_over(view, j, offsets):
        for dx, dy in offsets:
            block = view.at[owner(dx, dy)]
            push(block, block, j, d2d.at[j], sibling)

    def event0(j):
        def go(src, view):
            for target in (xp, xm, yp, ym):
                push(src, view.at[me], j, recv.at[0, j], target)
            push(src, view.at[me], j, d2d.at[j], sibling)
        own_by_kind(j, go)

    def event1(j):
        def go(view):
            wait_shards(view, 4, recv.at[0, j])
            relay(view, j, 1, (
                ((1, 0), "left", xp), ((-1, 0), "right", xm), ((0, 1), "left", yp), ((0, -1), "right", ym),
                ((0, 1), "bottom", xp), ((0, 1), "bottom", xm), ((1, 0), "top", yp), ((1, 0), "top", ym),
                ((0, -1), "bottom", xp), ((0, -1), "bottom", xm), ((-1, 0), "top", yp), ((-1, 0), "top", ym)))
            hand_over(view, j, ((1, 0), (-1, 0), (0, 1), (0, -1)))
        by_kind(j, go)

    def event2(j):
        def go(view):
            wait_shards(view, 6, recv.at[1, j])
            relay(view, j, 2, (
                ((0, 2), "bottom", xp), ((0, 2), "bottom", xm), ((2, 0), "top", yp), ((2, 0), "top", ym),
                ((1, 1), "c", xp), ((-1, 1), "d", xm), ((1, 1), "a", yp), ((1, -1), "b", ym),
                ((1, -1), "c", xp), ((-1, -1), "d", xm), ((-1, 1), "a", yp), ((-1, -1), "b", ym)))
            hand_over(view, j, ((2, 0), (0, 2), (1, 1), (1, -1), (-1, 1), (-1, -1)))
        by_kind(j, go)

    def event3(j):
        def go(view):
            wait_shards(view, 4, recv.at[2, j])
            relay(view, j, 3, (((1, 2), "c", xp), ((-1, 2), "d", xm), ((2, 1), "a", yp), ((2, -1), "b", ym)))
            hand_over(view, j, ((2, 1), (2, -1), (1, 2), (-1, 2)))
        by_kind(j, go)

    def event4(j):
        def go(view):
            wait_shards(view, 1, recv.at[3, j])
            hand_over(view, j, ((2, 2),))
        by_kind(j, go)

    late = chunks - LATE

    def when_chunk(event, j):
        pl.when((j >= 0) & (j < chunks))(lambda: event(j))

    def early(t, far, near):
        return jnp.where(t + far < late, t + far, jnp.where(t + near >= late, t + near, chunks))

    def pump(t):
        when_chunk(event3, t)
        when_chunk(event2, t + 1)
        when_chunk(event1, early(t, 3, 2))
        when_chunk(event0, early(t, 5, 3))

    fold = ff // width
    band_rows = width * n // ff

    def fetch(view, own, put, sem, j):
        if RUN_COMM:
            wait_shards(view, n // 2, d2d.at[j])

        def one(d):
            @pl.when(d != me)
            def _():
                pltpu.make_async_copy(view.at[d], put(d), sem).start()

            @pl.when(d == me)
            def _():
                pltpu.make_async_copy(own, put(d), sem).start()

        fori(0, n, one)

    def fetch_chunk(j):
        slot, sem = ws.at[j % SLOTS], load_sem.at[j % SLOTS]

        def go(own, view):
            rows, cols = view.shape[1], view.shape[2]
            if rows * n == width:
                def put(d):
                    return slot.at[pl.ds(pl.multiple_of(d * rows, rows), rows), pl.ds(0, cols)]
            else:
                def put(d):
                    return slot.at[pl.ds(pl.multiple_of((d % band_rows) * rows, rows), rows),
                                   pl.ds(pl.multiple_of((d // band_rows) * cols, cols), cols)]
            fetch(view, own, put, sem, j)

        own_by_kind(j, go, vectors=False)

    def wait_chunk(j, cols):
        part = ws.at[j % SLOTS].at[:, pl.ds(0, cols)]
        pltpu.make_async_copy(part, part, load_sem.at[j % SLOTS]).wait()

    def spread_vectors():
        fetch(g_vec, vp16, lambda d: gv.at[pl.ds(pl.multiple_of(d * 2 * VROWS, 2 * VROWS), 2 * VROWS), :], vec_sem, 0)
        pltpu.make_async_copy(gv, gv, vec_sem).wait()
        rows = gv.shape[0]
        for layer in range(layers):
            for k, part, total in ((LN1G, width // n, width), (LN1B, width // n, width), (LN2G, width // n, width),
                                   (LN2B, width // n, width), (BOUT, width // n, width), (BPROJ, width // n, width),
                                   (BATTN, qkv // n, qkv), (BFC, ff // n, ff)):
                dd = lax.broadcasted_iota(jnp.int32, (n, rows), 0)
                rr = lax.broadcasted_iota(jnp.int32, (n, rows), 1)
                pick = jnp.where(rr == dd * (2 * VROWS) + (layer * VROWS + k), 1.0, 0.0).astype(BF16)
                piece = jnp.dot(pick, gv[...], preferred_element_type=F32).astype(BF16)
                block = total if total <= qkv else width
                for start in range(0, total, block):
                    pos = lax.broadcasted_iota(jnp.int32, (1, block), 1).astype(F32) + float(start)
                    whose = jnp.floor((pos + 0.5) * (1.0 / part))
                    lane = pos - whose * float(part)
                    cc = lax.broadcasted_iota(jnp.int32, (VCOLS, block), 0).astype(F32)
                    place = jnp.where(cc == lane, 1.0, 0.0).astype(BF16)
                    wide = jnp.dot(piece, place, preferred_element_type=F32)
                    di = lax.broadcasted_iota(jnp.int32, (n, block), 0).astype(F32)
                    row = jnp.sum(jnp.where(di == whose, wide, 0.0), axis=0, keepdims=True)
                    vecs[layer, k:k + 1, start:start + block] = row

    def layer_norm(layer, gain_row, shift_row):
        tile, unroll = 16, 4

        def one(i):
            for u in range(unroll):
                rows = pl.ds(pl.multiple_of((i * unroll + u) * tile, tile), tile)
                wide = x[rows, :].astype(F32)
                mean = jnp.mean(wide, axis=-1, keepdims=True)
                centred = wide - mean
                variance = jnp.mean(centred * centred, axis=-1, keepdims=True)
                normed = centred * lax.rsqrt(variance + EPS)
                gain = vecs[layer, gain_row:gain_row + 1, 0:width]
                shift = vecs[layer, shift_row:shift_row + 1, 0:width]
                h[rows, :] = (normed * gain + shift).astype(BF16)

        fori(0, tokens // (tile * unroll), one)

    m_tile = seq

    def stage_qkv(layer, half):
        j = 1 + layer * per_layer
        n_tile = 2 * head
        tiles = qkv // n_tile

        @pl.when(half == 0)
        def _():
            @pl.when(layer > 0)
            def _():
                layer_norm(layer, LN1G, LN1B)
            wait_chunk(j, qkv)

        def one(i):
            cols = pl.ds(pl.multiple_of(i * n_tile, n_tile), n_tile)
            bias = vecs[layer, BATTN:BATTN + 1, cols]
            for m in range(tokens // m_tile):
                rows = slice(m * m_tile, (m + 1) * m_tile)
                acc = jnp.dot(h[rows, :], ws[j % SLOTS, :, cols], preferred_element_type=F32)
                inner[rows, cols] = (acc + bias).astype(BF16)

        fori(half * (tiles // 2), tiles // 2 + half * (tiles - tiles // 2), one)

        @pl.when(half == 1)
        def _():
            for p in range(prompts):
                rows = pl.ds(p * seq, seq)
                pltpu.make_async_copy(inner.at[rows, pl.ds(width, head)], kc.at[p, layer], cache_sem.at[2 * p]).start()
                pltpu.make_async_copy(inner.at[rows, pl.ds(width + head, head)], vc.at[p, layer], cache_sem.at[2 * p + 1]).start()

    def wait_caches(layer):
        for p in range(prompts):
            rows = pl.ds(p * seq, seq)
            pltpu.make_async_copy(inner.at[rows, pl.ds(width, head)], kc.at[p, layer], cache_sem.at[2 * p]).wait()
            pltpu.make_async_copy(inner.at[rows, pl.ds(width + head, head)], vc.at[p, layer], cache_sem.at[2 * p + 1]).wait()

    q_tile = 128
    group = 4
    to_log2 = head ** -0.5 * math.log2(math.e)
    masked = -1e30 * head ** 0.5

    def attention(p):
        length = lens[p]
        start = p * seq

        def one(i):
            for b in range(seq // q_tile):
                keys = (b + 1) * q_tile
                rows = slice(start + b * q_tile, start + (b + 1) * q_tile)
                cols = [pl.ds(pl.multiple_of((i * group + u) * head, head), head) for u in range(group)]
                query = jnp.concatenate([inner[rows, c] for c in cols], axis=0)
                kk = inner[start:start + keys, width:width + head]
                vv = inner[start:start + keys, width + head:width + 2 * head]
                scores = lax.dot_general(query, kk, (((1,), (1,)), ((), ())), preferred_element_type=F32)
                ki = lax.broadcasted_iota(jnp.int32, (q_tile, keys), 1)
                qi = lax.broadcasted_iota(jnp.int32, (q_tile, keys), 0) + b * q_tile
                allowed = (ki <= qi) & (ki < length)
                probs = []
                for u in range(group):
                    score = jnp.where(allowed, scores[u * q_tile:(u + 1) * q_tile, :], masked)
                    peak = jnp.max(score, axis=-1, keepdims=True)
                    e = jnp.exp2((score - peak) * to_log2)
                    probs.append((e * (1.0 / jnp.sum(e, axis=-1, keepdims=True))).astype(BF16))
                mixed = jnp.dot(jnp.concatenate(probs, axis=0), vv, preferred_element_type=F32).astype(BF16)
                for u in range(group):
                    h[rows, cols[u]] = mixed[u * q_tile:(u + 1) * q_tile, :]

        fori(0, heads // group, one)

    def stage_out(layer):
        j = 2 + layer * per_layer
        wait_chunk(j, width)
        n_tile = min(512, width)

        def one(i):
            cols = pl.ds(pl.multiple_of(i * n_tile, n_tile), n_tile)
            bias = vecs[layer, BOUT:BOUT + 1, cols]
            for m in range(tokens // m_tile):
                rows = slice(m * m_tile, (m + 1) * m_tile)
                acc = jnp.dot(h[rows, :], ws[j % SLOTS, :, cols], preferred_element_type=F32)
                x[rows, cols] = (x[rows, cols].astype(F32) + (acc + bias)).astype(BF16)

        fori(0, width // n_tile, one)

    def stage_fc(layer, unit):
        c, part = unit // 2, unit % 2
        base = c * fc_cols
        j = 3 + c + layer * per_layer
        pl.when(part == 0)(lambda: wait_chunk(j, fc_cols))
        n_tile = min(512, fc_cols)

        def one(i):
            cols = pl.ds(pl.multiple_of(i * n_tile, n_tile), n_tile)
            far = pl.ds(pl.multiple_of(base + i * n_tile, n_tile), n_tile)
            bias = vecs[layer, BFC:BFC + 1, far]
            for m in range(tokens // m_tile):
                rows = slice(m * m_tile, (m + 1) * m_tile)
                acc = jnp.dot(h[rows, :], ws[j % SLOTS, :, cols], preferred_element_type=F32) + bias
                inner[rows, far] = jax.nn.gelu(acc, approximate=True).astype(BF16)

        tiles = fc_cols // n_tile
        fori(part * (tiles // 2), tiles // 2 + part * (tiles - tiles // 2), one)

    def stage_proj(layer, c, half):
        base = c * pr_cols
        cols = pl.ds(pl.multiple_of(base, pr_cols), pr_cols)
        j = 3 + FC_PARTS + c + layer * per_layer
        pl.when(half == 0)(lambda: wait_chunk(j, width))
        bias = vecs[layer, BPROJ:BPROJ + 1, cols]

        def one(m):
            rows = pl.ds(pl.multiple_of(m * m_tile, m_tile), m_tile)
            acc = bias
            for q in range(fold):
                acc = acc + jnp.dot(inner[rows, q * width:(q + 1) * width], ws[j % SLOTS, :, q * pr_cols:(q + 1) * pr_cols],
                                    preferred_element_type=F32)
            x[rows, cols] = (x[rows, cols].astype(F32) + acc).astype(BF16)

        tiles = tokens // m_tile
        cut = tiles - tiles // 2
        fori(half * cut, cut + half * (tiles - cut), one)

        @pl.when((layer == layers - 1) & (half == 1))
        def _():
            for p in range(prompts):
                pltpu.make_async_copy(x.at[pl.ds(p * seq, seq), cols], out.at[p, :, cols], io_sem.at[0]).start()

    first_fc, first_proj = 3, 2 + FC_PARTS

    def compute(t, half):
        layer, r = (t - 2) // per_layer, (t - 2) % per_layer
        live = (t >= 2) & (t < 2 + layers * per_layer)

        @pl.when((t == 1) & (half == 0))
        def _():
            spread_vectors()
            for p in range(prompts):
                pltpu.make_async_copy(tok.at[p], x.at[pl.ds(p * seq, seq), :], io_sem.at[p]).wait()

        @pl.when((t == 1) & (half == 1))
        def _():
            layer_norm(0, LN1G, LN1B)

        @pl.when(live & (r == 0))
        def _():
            stage_qkv(layer, half)

        for p in range(prompts):
            pl.when(live & (r == 1) & (half == (p == prompts - 1)))(functools.partial(attention, p))

        @pl.when(live & (r == 2) & (half == 0))
        def _():
            wait_caches(layer)
            stage_out(layer)

        @pl.when(live & (r == 2) & (half == 1))
        def _():
            layer_norm(layer, LN2G, LN2B)

        @pl.when(live & (r >= first_fc) & (r < first_proj))
        def _():
            lo = 3 * (r - first_fc) + 2 * half
            hi = jnp.minimum(lo + 2 - half, 2 * FC_PARTS)
            fori(lo, hi, lambda unit: stage_fc(layer, unit))

        @pl.when(live & (r >= first_proj))
        def _():
            stage_proj(layer, r - first_proj, half)

    def slot_step(i):
        t, half = i // 2 - 5, i % 2
        if RUN_COMM:
            pl.when(half == 0)(lambda: pump(t))
            pl.when(half == 1)(lambda: when_chunk(event4, t))
        if RUN_COMPUTE:
            pl.when((half == 1) & (t >= 1) & (t < chunks))(lambda: fetch_chunk(t))
            compute(t, half)

    if not RUN_COMPUTE:
        for p in range(prompts):
            pltpu.make_async_copy(tok.at[p], x.at[pl.ds(p * seq, seq), :], io_sem.at[p]).wait()
            pltpu.make_async_copy(x.at[pl.ds(p * seq, seq), :], out.at[p], io_sem.at[0]).start()
    fori(0, 2 * (chunks + 6), slot_step)

    if not RUN_COMPUTE and RUN_COMM:
        fori(0, chunks, lambda j: by_kind(j, lambda view: wait_shards(view, n // 2, d2d.at[j])))
    if RUN_COMM:
        fori(0, chunks, lambda j: by_kind(j, lambda view: wait_shards(view, n - 1, sent.at[j])))
    pltpu.make_async_copy(x, x, io_sem.at[0]).wait()


def hand_out(a, b, c, a_out, b_out, c_out):
    a_out[...] = a[...]
    b_out[...] = b[...]
    c_out[...] = c[...]


def solution(mesh):
    n = mesh.shape["dp"]
    tok_spec = P(('part', 'dp'), None, None)
    len_spec = P(('part', 'dp'))
    cache_spec = P(('part', 'dp'), None, None, None)
    vec_spec = P(None, 'dp')
    mat_spec = P(None, 'dp', None)

    def local(tokens, lengths, ln1_gain, ln1_bias, w_attn, b_attn, w_out, b_out, ln2_gain, ln2_bias, w_fc, b_fc, w_proj, b_proj):
        layers = w_attn.shape[0]
        prompts, seq, width = tokens.shape
        qkv = w_attn.shape[2]
        head = (qkv - width) // 2
        ff = w_fc.shape[2]
        rows = prompts * seq
        per_layer = 2 + FC_PARTS + PROJ_PARTS
        chunks = 1 + layers * per_layer
        r_in, r_ff = width // n, ff // n
        assert ff // FC_PARTS == width and layers * VROWS <= 2 * VROWS
        anywhere = pl.BlockSpec(memory_space=pl.ANY)
        vmem = pl.BlockSpec(memory_space=pltpu.VMEM)
        smem = pl.BlockSpec(memory_space=pltpu.SMEM)
        sds = jax.ShapeDtypeStruct
        cache = sds((prompts, layers, seq, head), BF16)
        results = pl.pallas_call(
            functools.partial(kernel, n),
            out_shape=(sds(tokens.shape, BF16), cache, cache,
                       sds((n, 2 * VROWS, VCOLS), BF16),
                       sds((layers, n, r_in, qkv), BF16),
                       sds((layers, 1 + FC_PARTS, n, r_in, width), BF16),
                       sds((layers, PROJ_PARTS, n, r_ff, width // PROJ_PARTS), BF16)),
            in_specs=[anywhere, smem] + [vmem] * 8 + [anywhere] * 4,
            out_specs=(anywhere,) * 7,
            scratch_shapes=[
                pltpu.VMEM((rows, width), BF16),
                pltpu.VMEM((rows, width), BF16),
                pltpu.VMEM((rows, ff), BF16),
                pltpu.VMEM((SLOTS, width, qkv), BF16),
                pltpu.VMEM((layers, 8, ff), F32),
                pltpu.VMEM((2 * VROWS, VCOLS), F32),
                pltpu.VMEM((2 * VROWS, VCOLS), BF16),
                pltpu.VMEM((n * 2 * VROWS, VCOLS), BF16),
                pltpu.SemaphoreType.DMA((4, chunks)),
                pltpu.SemaphoreType.DMA((chunks,)),
                pltpu.SemaphoreType.DMA((chunks,)),
                pltpu.SemaphoreType.DMA((SLOTS,)),
                pltpu.SemaphoreType.DMA,
                pltpu.SemaphoreType.DMA((prompts,)),
                pltpu.SemaphoreType.DMA((2 * prompts,)),
            ],
            compiler_params=pltpu.CompilerParams(collective_id=0, has_side_effects=True, vmem_limit_bytes=67043328),
            name="gather_layers",
        )(tokens, lengths, ln1_gain, ln1_bias, b_attn, b_out, ln2_gain, ln2_bias, b_fc, b_proj, w_attn, w_out, w_fc, w_proj)
        block = lambda shape: pl.BlockSpec((1,) + shape[1:], lambda i: (i,) + (0,) * (len(shape) - 1))
        shapes = (tokens.shape, cache.shape, cache.shape)
        return pl.pallas_call(
            hand_out,
            grid=(prompts,),
            out_shape=(sds(tokens.shape, BF16), cache, cache),
            in_specs=[block(shape) for shape in shapes],
            out_specs=tuple(block(shape) for shape in shapes),
            compiler_params=pltpu.CompilerParams(dimension_semantics=("arbitrary",)),
            name="hand_out",
        )(*results[:3])

    return jax.shard_map(local, mesh=mesh,
                         in_specs=(tok_spec, len_spec, vec_spec, vec_spec, mat_spec, vec_spec, mat_spec, vec_spec, vec_spec, vec_spec, mat_spec, vec_spec, mat_spec, vec_spec),
                         out_specs=(tok_spec, cache_spec, cache_spec), check_vma=False)
```

```python
import functools
import math

import jax
import jax.numpy as jnp
from jax import lax
from jax.experimental import pallas as pl
from jax.experimental.pallas import tpu as pltpu
from jax.sharding import PartitionSpec as P

EPS = 1e-5
F32 = jnp.float32
BF16 = jnp.bfloat16
FC_PARTS = 4
PROJ_PARTS = 4
LAST_WIDE = 3
VROWS = 16
VCOLS = 256
SLOTS = 3
LATE = 2
RUN_COMM = True
RUN_COMPUTE = True

LN1G, LN1B, LN2G, LN2B, BOUT, BPROJ, BATTN, BFC = range(8)


def fori(lower, upper, body):
    lax.fori_loop(lower, upper, lambda i, c: (body(i), c)[1], 0)


def kernel(n, tok, lens, ln1g, ln1b, b_attn, b_out, ln2g, ln2b, b_fc, b_proj, w_attn, w_out, w_fc, w_proj,
           out, kc, vc, g_vec, g_attn, g_main, g_proj,
           x, h, inner, ws, vecs, vp, vp16, gv,
           recv, d2d, sent, load_sem, vec_sem, io_sem, cache_sem):
    layers = w_attn.shape[0]
    prompts, seq, width = tok.shape
    head = kc.shape[-1]
    heads = width // head
    ff = b_fc.shape[1] * n
    tokens = prompts * seq
    qkv = width + 2 * head
    per_layer = 2 + FC_PARTS + PROJ_PARTS
    chunks = 1 + layers * per_layer + (PROJ_PARTS - LAST_WIDE)
    fc_cols = ff // FC_PARTS
    pr_cols = width // PROJ_PARTS
    half_cols = pr_cols // 2

    side = math.isqrt(n // 2)
    me = lax.axis_index("dp")
    core = me % 2
    px = (me // 2) % side
    py = me // (2 * side)

    def dev(dx, dy):
        return (((py + dy + side) % side) * side + (px + dx + side) % side) * 2 + core

    sibling = me + 1 - 2 * core
    xp, xm, yp, ym = dev(1, 0), dev(-1, 0), dev(0, 1), dev(0, -1)

    def owner(dx, dy):
        return dev(-dx, -dy)

    vp[...] = jnp.zeros_like(vp)
    for k, ref in ((LN1G, ln1g), (LN1B, ln1b), (LN2G, ln2g), (LN2B, ln2b), (BOUT, b_out), (BPROJ, b_proj), (BATTN, b_attn), (BFC, b_fc)):
        wide = ref[...].astype(F32)
        for layer in range(layers):
            vp[layer * VROWS + k:layer * VROWS + k + 1, 0:ref.shape[1]] = wide[layer:layer + 1, :]
    vp16[...] = vp[...].astype(BF16)

    for p in range(prompts):
        pltpu.make_async_copy(tok.at[p], x.at[pl.ds(p * seq, seq), :], io_sem.at[p]).start()

    barrier = pltpu.get_barrier_semaphore()
    for other in (xp, xm, yp, ym, sibling):
        pl.semaphore_signal(barrier, inc=1, device_id={"dp": other})
    pl.semaphore_wait(barrier, 5)

    def layer_of(j):
        layer = jnp.minimum((j - 1) // per_layer, layers - 1)
        return layer, j - 1 - layer * per_layer

    def is_narrow(layer, r):
        return (layer == layers - 1) & (r >= 2 + FC_PARTS + LAST_WIDE)

    def narrow_part(r):
        q = r - (2 + FC_PARTS + LAST_WIDE)
        return LAST_WIDE + q // 2, pl.ds(pl.multiple_of((q % 2) * half_cols, half_cols), half_cols)

    def by_kind(j, fn):
        layer, r = layer_of(j)

        @pl.when(j == 0)
        def _():
            fn(g_vec)

        @pl.when((j > 0) & (r == 0))
        def _():
            fn(g_attn.at[layer])

        @pl.when((j > 0) & (r >= 1) & (r < 2 + FC_PARTS))
        def _():
            fn(g_main.at[layer, r - 1])

        narrow = is_narrow(layer, r)

        @pl.when((j > 0) & (r >= 2 + FC_PARTS) & jnp.logical_not(narrow))
        def _():
            fn(g_proj.at[layer, r - 2 - FC_PARTS])

        @pl.when((j > 0) & narrow)
        def _():
            c, cols = narrow_part(r)
            fn(g_proj.at[layer, c].at[:, :, cols])

    def own_by_kind(j, fn, vectors=True):
        layer, r = layer_of(j)

        if vectors:
            @pl.when(j == 0)
            def _():
                fn(vp16, g_vec)

        @pl.when((j > 0) & (r == 0))
        def _():
            fn(w_attn.at[layer], g_attn.at[layer])

        @pl.when((j > 0) & (r == 1))
        def _():
            fn(w_out.at[layer], g_main.at[layer, 0])

        @pl.when((j > 0) & (r >= 2) & (r < 2 + FC_PARTS))
        def _():
            c = r - 2
            fn(w_fc.at[layer, :, pl.ds(pl.multiple_of(c * fc_cols, fc_cols), fc_cols)], g_main.at[layer, r - 1])

        narrow = is_narrow(layer, r)

        @pl.when((j > 0) & narrow)
        def _():
            c, cols = narrow_part(r)
            far = pl.ds(pl.multiple_of(c * pr_cols + cols.start, half_cols), half_cols)
            fn(w_proj.at[layer, :, far], g_proj.at[layer, c].at[:, :, cols])

        @pl.when((j > 0) & (r >= 2 + FC_PARTS) & jnp.logical_not(narrow))
        def _():
            c = r - 2 - FC_PARTS
            fn(w_proj.at[layer, :, pl.ds(pl.multiple_of(c * pr_cols, pr_cols), pr_cols)], g_proj.at[layer, c])

    def wait_shards(view, count, sem):
        part = view.at[pl.ds(0, count)]
        pltpu.make_async_copy(part, part, sem).wait()

    def push(src, dst, j, sem, device):
        pltpu.make_async_remote_copy(src_ref=src, dst_ref=dst, send_sem=sent.at[j], recv_sem=sem, device_id={"dp": device}).start()

    def relay(view, j, event, moves):
        rows, cols = view.shape[1], view.shape[2]
        half_r, half_c = rows // 2, cols // 2
        whole_r, whole_c = pl.ds(0, rows), pl.ds(0, cols)
        top, bottom = pl.ds(0, half_r), pl.ds(half_r, half_r)
        left, right = pl.ds(0, half_c), pl.ds(half_c, half_c)
        cut = dict(top=(top, whole_c), bottom=(bottom, whole_c), left=(whole_r, left), right=(whole_r, right),
                   a=(top, left), b=(top, right), c=(bottom, left), d=(bottom, right))
        for (dx, dy), name, target in moves:
            block = view.at[owner(dx, dy)].at[cut[name]]
            push(block, block, j, recv.at[event, j], target)

    def hand_over(view, j, offsets):
        for dx, dy in offsets:
            block = view.at[owner(dx, dy)]
            push(block, block, j, d2d.at[j], sibling)

    def event0(j):
        def go(src, view):
            for target in (xp, xm, yp, ym):
                push(src, view.at[me], j, recv.at[0, j], target)
            push(src, view.at[me], j, d2d.at[j], sibling)
        own_by_kind(j, go)

    def event1(j):
        def go(view):
            wait_shards(view, 4, recv.at[0, j])
            relay(view, j, 1, (
                ((1, 0), "left", xp), ((-1, 0), "right", xm), ((0, 1), "left", yp), ((0, -1), "right", ym),
                ((0, 1), "bottom", xp), ((0, 1), "bottom", xm), ((1, 0), "top", yp), ((1, 0), "top", ym),
                ((0, -1), "bottom", xp), ((0, -1), "bottom", xm), ((-1, 0), "top", yp), ((-1, 0), "top", ym)))
            hand_over(view, j, ((1, 0), (-1, 0), (0, 1), (0, -1)))
        by_kind(j, go)

    def event2(j):
        def go(view):
            wait_shards(view, 6, recv.at[1, j])
            relay(view, j, 2, (
                ((0, 2), "bottom", xp), ((0, 2), "bottom", xm), ((2, 0), "top", yp), ((2, 0), "top", ym),
                ((1, 1), "c", xp), ((-1, 1), "d", xm), ((1, 1), "a", yp), ((1, -1), "b", ym),
                ((1, -1), "c", xp), ((-1, -1), "d", xm), ((-1, 1), "a", yp), ((-1, -1), "b", ym)))
            hand_over(view, j, ((2, 0), (0, 2), (1, 1), (1, -1), (-1, 1), (-1, -1)))
        by_kind(j, go)

    def event3(j):
        def go(view):
            wait_shards(view, 4, recv.at[2, j])
            relay(view, j, 3, (((1, 2), "c", xp), ((-1, 2), "d", xm), ((2, 1), "a", yp), ((2, -1), "b", ym)))
            hand_over(view, j, ((2, 1), (2, -1), (1, 2), (-1, 2)))
        by_kind(j, go)

    def event4(j):
        def go(view):
            wait_shards(view, 1, recv.at[3, j])
            hand_over(view, j, ((2, 2),))
        by_kind(j, go)

    late = chunks - LATE

    def when_chunk(event, j):
        pl.when((j >= 0) & (j < chunks))(lambda: event(j))

    def early(t, far, near):
        return jnp.where(t + far < late, t + far, jnp.where(t + near >= late, t + near, chunks))

    def pump(t):
        when_chunk(event3, t)
        when_chunk(event2, t + 1)
        when_chunk(event1, early(t, 3, 2))
        when_chunk(event0, early(t, 5, 3))

    fold = ff // width
    band_rows = width * n // ff

    def fetch(view, own, put, sem, j):
        if RUN_COMM:
            wait_shards(view, n // 2, d2d.at[j])

        def one(d):
            @pl.when(d != me)
            def _():
                pltpu.make_async_copy(view.at[d], put(d), sem).start()

            @pl.when(d == me)
            def _():
                pltpu.make_async_copy(own, put(d), sem).start()

        fori(0, n, one)

    def fetch_chunk(j):
        slot, sem = ws.at[j % SLOTS], load_sem.at[j % SLOTS]

        def go(own, view):
            rows, cols = view.shape[1], view.shape[2]
            if rows * n == width:
                def put(d):
                    return slot.at[pl.ds(pl.multiple_of(d * rows, rows), rows), pl.ds(0, cols)]
            else:
                def put(d):
                    return slot.at[pl.ds(pl.multiple_of((d % band_rows) * rows, rows), rows),
                                   pl.ds(pl.multiple_of((d // band_rows) * cols, cols), cols)]
            fetch(view, own, put, sem, j)

        own_by_kind(j, go, vectors=False)

    def wait_chunk(j, cols):
        part = ws.at[j % SLOTS].at[:, pl.ds(0, cols)]
        pltpu.make_async_copy(part, part, load_sem.at[j % SLOTS]).wait()

    def spread_vectors():
        fetch(g_vec, vp16, lambda d: gv.at[pl.ds(pl.multiple_of(d * 2 * VROWS, 2 * VROWS), 2 * VROWS), :], vec_sem, 0)
        pltpu.make_async_copy(gv, gv, vec_sem).wait()
        rows = gv.shape[0]
        for layer in range(layers):
            for k, part, total in ((LN1G, width // n, width), (LN1B, width // n, width), (LN2G, width // n, width),
                                   (LN2B, width // n, width), (BOUT, width // n, width), (BPROJ, width // n, width),
                                   (BATTN, qkv // n, qkv), (BFC, ff // n, ff)):
                dd = lax.broadcasted_iota(jnp.int32, (n, rows), 0)
                rr = lax.broadcasted_iota(jnp.int32, (n, rows), 1)
                pick = jnp.where(rr == dd * (2 * VROWS) + (layer * VROWS + k), 1.0, 0.0).astype(BF16)
                piece = jnp.dot(pick, gv[...], preferred_element_type=F32).astype(BF16)
                block = total if total <= qkv else width
                for start in range(0, total, block):
                    pos = lax.broadcasted_iota(jnp.int32, (1, block), 1).astype(F32) + float(start)
                    whose = jnp.floor((pos + 0.5) * (1.0 / part))
                    lane = pos - whose * float(part)
                    cc = lax.broadcasted_iota(jnp.int32, (VCOLS, block), 0).astype(F32)
                    place = jnp.where(cc == lane, 1.0, 0.0).astype(BF16)
                    wide = jnp.dot(piece, place, preferred_element_type=F32)
                    di = lax.broadcasted_iota(jnp.int32, (n, block), 0).astype(F32)
                    row = jnp.sum(jnp.where(di == whose, wide, 0.0), axis=0, keepdims=True)
                    vecs[layer, k:k + 1, start:start + block] = row

    def layer_norm(layer, gain_row, shift_row):
        tile, unroll = 16, 4

        def one(i):
            for u in range(unroll):
                rows = pl.ds(pl.multiple_of((i * unroll + u) * tile, tile), tile)
                wide = x[rows, :].astype(F32)
                mean = jnp.mean(wide, axis=-1, keepdims=True)
                centred = wide - mean
                variance = jnp.mean(centred * centred, axis=-1, keepdims=True)
                normed = centred * lax.rsqrt(variance + EPS)
                gain = vecs[layer, gain_row:gain_row + 1, 0:width]
                shift = vecs[layer, shift_row:shift_row + 1, 0:width]
                h[rows, :] = (normed * gain + shift).astype(BF16)

        fori(0, tokens // (tile * unroll), one)

    m_tile = seq

    def stage_qkv(layer, half):
        j = 1 + layer * per_layer
        n_tile = 2 * head
        tiles = qkv // n_tile

        @pl.when(half == 0)
        def _():
            @pl.when(layer > 0)
            def _():
                layer_norm(layer, LN1G, LN1B)
            wait_chunk(j, qkv)

        def one(i):
            cols = pl.ds(pl.multiple_of(i * n_tile, n_tile), n_tile)
            bias = vecs[layer, BATTN:BATTN + 1, cols]
            for m in range(tokens // m_tile):
                rows = slice(m * m_tile, (m + 1) * m_tile)
                acc = jnp.dot(h[rows, :], ws[j % SLOTS, :, cols], preferred_element_type=F32)
                inner[rows, cols] = (acc + bias).astype(BF16)

        fori(half * (tiles // 2), tiles // 2 + half * (tiles - tiles // 2), one)

        @pl.when(half == 1)
        def _():
            for p in range(prompts):
                rows = pl.ds(p * seq, seq)
                pltpu.make_async_copy(inner.at[rows, pl.ds(width, head)], kc.at[p, layer], cache_sem.at[2 * p]).start()
                pltpu.make_async_copy(inner.at[rows, pl.ds(width + head, head)], vc.at[p, layer], cache_sem.at[2 * p + 1]).start()

    def wait_caches(layer):
        for p in range(prompts):
            rows = pl.ds(p * seq, seq)
            pltpu.make_async_copy(inner.at[rows, pl.ds(width, head)], kc.at[p, layer], cache_sem.at[2 * p]).wait()
            pltpu.make_async_copy(inner.at[rows, pl.ds(width + head, head)], vc.at[p, layer], cache_sem.at[2 * p + 1]).wait()

    q_tile = 128
    group = 4
    to_log2 = head ** -0.5 * math.log2(math.e)
    masked = -1e30 * head ** 0.5

    def attention(p):
        length = lens[p]
        start = p * seq

        def one(i):
            for b in range(seq // q_tile):
                keys = (b + 1) * q_tile
                rows = slice(start + b * q_tile, start + (b + 1) * q_tile)
                cols = [pl.ds(pl.multiple_of((i * group + u) * head, head), head) for u in range(group)]
                query = jnp.concatenate([inner[rows, c] for c in cols], axis=0)
                kk = inner[start:start + keys, width:width + head]
                vv = inner[start:start + keys, width + head:width + 2 * head]
                scores = lax.dot_general(query, kk, (((1,), (1,)), ((), ())), preferred_element_type=F32)
                ki = lax.broadcasted_iota(jnp.int32, (q_tile, keys), 1)
                qi = lax.broadcasted_iota(jnp.int32, (q_tile, keys), 0) + b * q_tile
                allowed = (ki <= qi) & (ki < length)
                probs = []
                for u in range(group):
                    score = jnp.where(allowed, scores[u * q_tile:(u + 1) * q_tile, :], masked)
                    peak = jnp.max(score, axis=-1, keepdims=True)
                    e = jnp.exp2((score - peak) * to_log2)
                    probs.append((e * (1.0 / jnp.sum(e, axis=-1, keepdims=True))).astype(BF16))
                mixed = jnp.dot(jnp.concatenate(probs, axis=0), vv, preferred_element_type=F32).astype(BF16)
                for u in range(group):
                    h[rows, cols[u]] = mixed[u * q_tile:(u + 1) * q_tile, :]

        fori(0, heads // group, one)

    def stage_out(layer):
        j = 2 + layer * per_layer
        wait_chunk(j, width)
        n_tile = min(512, width)

        def one(i):
            cols = pl.ds(pl.multiple_of(i * n_tile, n_tile), n_tile)
            bias = vecs[layer, BOUT:BOUT + 1, cols]
            for m in range(tokens // m_tile):
                rows = slice(m * m_tile, (m + 1) * m_tile)
                acc = jnp.dot(h[rows, :], ws[j % SLOTS, :, cols], preferred_element_type=F32)
                x[rows, cols] = (x[rows, cols].astype(F32) + (acc + bias)).astype(BF16)

        fori(0, width // n_tile, one)

    def stage_fc(layer, unit):
        c, part = unit // 2, unit % 2
        base = c * fc_cols
        j = 3 + c + layer * per_layer
        pl.when(part == 0)(lambda: wait_chunk(j, fc_cols))
        n_tile = min(512, fc_cols)

        def one(i):
            cols = pl.ds(pl.multiple_of(i * n_tile, n_tile), n_tile)
            far = pl.ds(pl.multiple_of(base + i * n_tile, n_tile), n_tile)
            bias = vecs[layer, BFC:BFC + 1, far]
            for m in range(tokens // m_tile):
                rows = slice(m * m_tile, (m + 1) * m_tile)
                acc = jnp.dot(h[rows, :], ws[j % SLOTS, :, cols], preferred_element_type=F32) + bias
                inner[rows, far] = jax.nn.gelu(acc, approximate=True).astype(BF16)

        tiles = fc_cols // n_tile
        fori(part * (tiles // 2), tiles // 2 + part * (tiles - tiles // 2), one)

    def stage_proj(layer, c, half):
        base = c * pr_cols
        cols = pl.ds(pl.multiple_of(base, pr_cols), pr_cols)
        j = 3 + FC_PARTS + c + layer * per_layer
        pl.when(half == 0)(lambda: wait_chunk(j, width))
        bias = vecs[layer, BPROJ:BPROJ + 1, cols]

        def one(m):
            rows = pl.ds(pl.multiple_of(m * m_tile, m_tile), m_tile)
            acc = bias
            for q in range(fold):
                acc = acc + jnp.dot(inner[rows, q * width:(q + 1) * width], ws[j % SLOTS, :, q * pr_cols:(q + 1) * pr_cols],
                                    preferred_element_type=F32)
            x[rows, cols] = (x[rows, cols].astype(F32) + acc).astype(BF16)

        tiles = tokens // m_tile
        cut = tiles - tiles // 2
        fori(half * cut, cut + half * (tiles - cut), one)

        @pl.when((layer == layers - 1) & (half == 1))
        def _():
            for p in range(prompts):
                pltpu.make_async_copy(x.at[pl.ds(p * seq, seq), cols], out.at[p, :, cols], io_sem.at[0]).start()

    def stage_proj_narrow(layer, r):
        c, cols = narrow_part(r)
        far = pl.ds(pl.multiple_of(c * pr_cols + cols.start, half_cols), half_cols)
        j = 1 + layer * per_layer + r
        wait_chunk(j, fold * half_cols)
        bias = vecs[layer, BPROJ:BPROJ + 1, far]
        for m in range(tokens // m_tile):
            rows = slice(m * m_tile, (m + 1) * m_tile)
            acc = bias
            for q in range(fold):
                acc = acc + jnp.dot(inner[rows, q * width:(q + 1) * width], ws[j % SLOTS, :, q * half_cols:(q + 1) * half_cols],
                                    preferred_element_type=F32)
            x[rows, far] = (x[rows, far].astype(F32) + acc).astype(BF16)
        for p in range(prompts):
            pltpu.make_async_copy(x.at[pl.ds(p * seq, seq), far], out.at[p, :, far], io_sem.at[0]).start()

    first_fc, first_proj = 3, 2 + FC_PARTS

    def compute(t, half):
        layer, r = layer_of(t - 1)
        live = (t >= 2) & (t < 1 + chunks)
        narrow = is_narrow(layer, r)

        @pl.when((t == 1) & (half == 0))
        def _():
            spread_vectors()
            for p in range(prompts):
                pltpu.make_async_copy(tok.at[p], x.at[pl.ds(p * seq, seq), :], io_sem.at[p]).wait()

        @pl.when((t == 1) & (half == 1))
        def _():
            layer_norm(0, LN1G, LN1B)

        @pl.when(live & (r == 0))
        def _():
            stage_qkv(layer, half)

        for p in range(prompts):
            pl.when(live & (r == 1) & (half == (p == prompts - 1)))(functools.partial(attention, p))

        @pl.when(live & (r == 2) & (half == 0))
        def _():
            wait_caches(layer)
            stage_out(layer)

        @pl.when(live & (r == 2) & (half == 1))
        def _():
            layer_norm(layer, LN2G, LN2B)

        @pl.when(live & (r >= first_fc) & (r < first_proj))
        def _():
            lo = 3 * (r - first_fc) + 2 * half
            hi = jnp.minimum(lo + 2 - half, 2 * FC_PARTS)
            fori(lo, hi, lambda unit: stage_fc(layer, unit))

        @pl.when(live & (r >= first_proj) & jnp.logical_not(narrow))
        def _():
            stage_proj(layer, r - first_proj, half)

        @pl.when(live & narrow & (half == 0))
        def _():
            stage_proj_narrow(layer, r)

    def slot_step(i):
        t, half = i // 2 - 5, i % 2
        if RUN_COMM:
            pl.when(half == 0)(lambda: pump(t))
            pl.when(half == 1)(lambda: when_chunk(event4, t))
        if RUN_COMPUTE:
            pl.when((half == 1) & (t >= 1) & (t < chunks))(lambda: fetch_chunk(t))
            compute(t, half)

    if not RUN_COMPUTE:
        for p in range(prompts):
            pltpu.make_async_copy(tok.at[p], x.at[pl.ds(p * seq, seq), :], io_sem.at[p]).wait()
            pltpu.make_async_copy(x.at[pl.ds(p * seq, seq), :], out.at[p], io_sem.at[0]).start()
    fori(0, 2 * (chunks + 6), slot_step)

    if not RUN_COMPUTE and RUN_COMM:
        fori(0, chunks, lambda j: by_kind(j, lambda view: wait_shards(view, n // 2, d2d.at[j])))
    if RUN_COMM:
        fori(0, chunks, lambda j: by_kind(j, lambda view: wait_shards(view, n - 1, sent.at[j])))
    pltpu.make_async_copy(x, x, io_sem.at[0]).wait()


def hand_out(a, b, c, a_out, b_out, c_out):
    a_out[...] = a[...]
    b_out[...] = b[...]
    c_out[...] = c[...]


def solution(mesh):
    n = mesh.shape["dp"]
    tok_spec = P(('part', 'dp'), None, None)
    len_spec = P(('part', 'dp'))
    cache_spec = P(('part', 'dp'), None, None, None)
    vec_spec = P(None, 'dp')
    mat_spec = P(None, 'dp', None)

    def local(tokens, lengths, ln1_gain, ln1_bias, w_attn, b_attn, w_out, b_out, ln2_gain, ln2_bias, w_fc, b_fc, w_proj, b_proj):
        layers = w_attn.shape[0]
        prompts, seq, width = tokens.shape
        qkv = w_attn.shape[2]
        head = (qkv - width) // 2
        ff = w_fc.shape[2]
        rows = prompts * seq
        per_layer = 2 + FC_PARTS + PROJ_PARTS
        chunks = 1 + layers * per_layer + (PROJ_PARTS - LAST_WIDE)
        r_in, r_ff = width // n, ff // n
        assert ff // FC_PARTS == width and layers * VROWS <= 2 * VROWS
        anywhere = pl.BlockSpec(memory_space=pl.ANY)
        vmem = pl.BlockSpec(memory_space=pltpu.VMEM)
        smem = pl.BlockSpec(memory_space=pltpu.SMEM)
        sds = jax.ShapeDtypeStruct
        cache = sds((prompts, layers, seq, head), BF16)
        results = pl.pallas_call(
            functools.partial(kernel, n),
            out_shape=(sds(tokens.shape, BF16), cache, cache,
                       sds((n, 2 * VROWS, VCOLS), BF16),
                       sds((layers, n, r_in, qkv), BF16),
                       sds((layers, 1 + FC_PARTS, n, r_in, width), BF16),
                       sds((layers, PROJ_PARTS, n, r_ff, width // PROJ_PARTS), BF16)),
            in_specs=[anywhere, smem] + [vmem] * 8 + [anywhere] * 4,
            out_specs=(anywhere,) * 7,
            scratch_shapes=[
                pltpu.VMEM((rows, width), BF16),
                pltpu.VMEM((rows, width), BF16),
                pltpu.VMEM((rows, ff), BF16),
                pltpu.VMEM((SLOTS, width, qkv), BF16),
                pltpu.VMEM((layers, 8, ff), F32),
                pltpu.VMEM((2 * VROWS, VCOLS), F32),
                pltpu.VMEM((2 * VROWS, VCOLS), BF16),
                pltpu.VMEM((n * 2 * VROWS, VCOLS), BF16),
                pltpu.SemaphoreType.DMA((4, chunks)),
                pltpu.SemaphoreType.DMA((chunks,)),
                pltpu.SemaphoreType.DMA((chunks,)),
                pltpu.SemaphoreType.DMA((SLOTS,)),
                pltpu.SemaphoreType.DMA,
                pltpu.SemaphoreType.DMA((prompts,)),
                pltpu.SemaphoreType.DMA((2 * prompts,)),
            ],
            compiler_params=pltpu.CompilerParams(collective_id=0, has_side_effects=True, vmem_limit_bytes=67043328),
            name="gather_layers",
        )(tokens, lengths, ln1_gain, ln1_bias, b_attn, b_out, ln2_gain, ln2_bias, b_fc, b_proj, w_attn, w_out, w_fc, w_proj)
        block = lambda shape: pl.BlockSpec((1,) + shape[1:], lambda i: (i,) + (0,) * (len(shape) - 1))
        shapes = (tokens.shape, cache.shape, cache.shape)
        return pl.pallas_call(
            hand_out,
            grid=(prompts,),
            out_shape=(sds(tokens.shape, BF16), cache, cache),
            in_specs=[block(shape) for shape in shapes],
            out_specs=tuple(block(shape) for shape in shapes),
            compiler_params=pltpu.CompilerParams(dimension_semantics=("arbitrary",)),
            name="hand_out",
        )(*results[:3])

    return jax.shard_map(local, mesh=mesh,
                         in_specs=(tok_spec, len_spec, vec_spec, vec_spec, mat_spec, vec_spec, mat_spec, vec_spec, vec_spec, vec_spec, mat_spec, vec_spec, mat_spec, vec_spec),
                         out_specs=(tok_spec, cache_spec, cache_spec), check_vma=False)
```
